128 devices in a mesh: items: 32 (over y, z, core), users: 4 (over x).
Axes of the slice: x: 4, y: 4, z: 4, core: 2. Of those that a mesh axis runs over, the one named last changes fastest.
Arguments:
- user_emb: bfloat16 [4096, 256], P('users', 'items'), as said below
- item_emb: bfloat16 [1048576, 256], P('items'), as said below
- target: int32 [4096], P('users'), may hold values from 0 to 1048575
- history: int32 [4096, 32], P('users'), may hold values from 0 to 1048575, as said below
Outputs:
- log_rank: float32 [4096], P('users')
- metrics: float32 [2], replicated
The draws below stay inside these ranges and needn't reach their ends.
Inputs may be any that keep to these rules, and one draw needn't show every extreme that they name: history[u, k] lies in [k * 32768, (k + 1) * 32768); a user's history entries are thus distinct. `item_emb`: rows of norm about one. `user_emb`: entries of order one.
All inputs are finite; a program needn't handle non-finite values.
Results may differ from the reference program's by a relative error of at most 0.0003.
Values may be sent and summed in bfloat16 or wider, within the bound.
A program may use at most 64 MiB of HBM per device.

```python
import jax
import jax.numpy as jnp
from jax import lax

D = 256
H = 32
ITEMS = 1048576
USERS = 4096


def item_row(base, row):
    return jax.random.normal(jax.random.fold_in(base, row), (D,), jnp.float32) / jnp.sqrt(float(D))


def shared_ints(key):
    target = jax.random.randint(jax.random.fold_in(key, 12), (USERS,), 0, ITEMS).astype(jnp.int32)
    stride = ITEMS // H
    offset = jax.random.randint(jax.random.fold_in(key, 13), (USERS, H), 0, stride).astype(jnp.int32)
    history = offset + (jnp.arange(H, dtype=jnp.int32) * stride)[None, :]
    return (target, history)


def draw_item_emb(key, part):
    base = jax.random.fold_in(key, 11)
    rows = jax.vmap(lambda r: item_row(base, r))(jnp.arange(ITEMS, dtype=jnp.int32))
    return rows.astype(jnp.bfloat16)


def draw_target(key, part):
    return shared_ints(key)[0]


def draw_history(key, part):
    return shared_ints(key)[1]


def draw_user_emb(key, part):
    base = jax.random.fold_in(key, 11)
    target, history = shared_ints(key)
    trow = jax.vmap(lambda r: item_row(base, r))(target)
    hrows = jax.vmap(jax.vmap(lambda r: item_row(base, r)))(history)
    noise = jax.random.normal(jax.random.fold_in(key, 14), (USERS, D), jnp.float32) * 0.6
    query = noise + 4.0 * trow + 2.5 * jnp.sum(hrows, axis=1)
    return query.astype(jnp.bfloat16)


def setup_inputs(seed: int = 0) -> dict:
    key_of = jax.random.split(jax.random.key(seed), 5)
    return {
        "user_emb": draw_user_emb(jax.random.fold_in(key_of[4], 71), 0),
        "item_emb": draw_item_emb(jax.random.fold_in(key_of[4], 71), 0),
        "target": draw_target(jax.random.fold_in(key_of[4], 71), 0),
        "history": draw_history(jax.random.fold_in(key_of[4], 71), 0),
    }


sharpness = 4.0


def reference(user_emb, item_emb, target, history):
    users = user_emb.astype(jnp.float32)
    items = item_emb.astype(jnp.float32)
    tscore = jnp.sum(users * items[target], axis=1)
    blk = min(ITEMS, 8192)
    nblk = ITEMS // blk
    blocks = items.reshape(nblk, blk, D)

    def step(total, rows):
        score = jnp.dot(users, rows.T, preferred_element_type=jnp.float32, precision=lax.Precision.HIGHEST)
        return total + jnp.sum(jax.nn.sigmoid(sharpness * (score - tscore[:, None])), axis=1), None

    total, _ = lax.scan(step, jnp.zeros((USERS,), jnp.float32), blocks)
    hrows = items[history]
    hscore = jnp.einsum("ud,uhd->uh", users, hrows, precision=lax.Precision.HIGHEST)
    seen_sum = jnp.sum(jax.nn.sigmoid(sharpness * (hscore - tscore[:, None])), axis=1)
    seen = jnp.any(history == target[:, None], axis=1)
    above = total - seen_sum - jnp.where(seen, 0.0, 0.5).astype(jnp.float32)
    rank = 1.0 + above
    log_rank = jnp.log(rank)
    hit = jax.nn.sigmoid(10.5 - rank)
    gain = hit / jnp.log2(1.0 + rank)
    metrics = jnp.stack([jnp.sum(hit), jnp.sum(gain)]) / USERS
    return log_rank, metrics
```

```python
import functools

import jax
import jax.numpy as jnp
from jax import lax
from jax.experimental import pallas as pl
from jax.experimental.pallas import tpu as pltpu
from jax.sharding import PartitionSpec as P

MESH = pl.DeviceIdType.MESH
SHARP_HALF = 2.0
ROWS = 2048
PARTS = 8


def to_peers(src, dst, send, recv, axis, me, n):
    for j in range(1, n):
        pltpu.make_async_remote_copy(
            src_ref=src, dst_ref=dst.at[me], send_sem=send, recv_sem=recv,
            device_id={axis: lax.rem(me + j, n)}, device_id_type=MESH,
        ).start()


def wait_bytes(ref, send, recv, axis):
    d = pltpu.make_async_remote_copy(
        src_ref=ref, dst_ref=ref, send_sem=send, recv_sem=recv,
        device_id={axis: 0}, device_id_type=MESH,
    )
    d.wait_recv()
    d.wait_send()


def kernel(ni, nu, u_ref, t_ref, h_ref, ts_ref, hh_ref, items_ref, out_ref, met_ref,
           buf, uall, U, gt, gh, hs, tval, lval, mval, trecv, lrecv, mrecv,
           isem, hsem, us, ur, ps, pr, tsd, trc, lsd, lrc, msd, mrc):
    n_tiles, sub, d = buf.shape
    n_rows = n_tiles * sub
    users = t_ref.shape[1]
    tiles = users // 256
    me = lax.axis_index("items")
    mx = lax.axis_index("users")
    core = lax.rem(me, 2)
    chip = me // 2
    chips = ni // 2
    partner = chip * 2 + 1 - core
    start = me * n_rows

    part = n_tiles // PARTS
    copies = [
        pltpu.make_async_copy(items_ref.at[pl.ds(p * part, part)], buf.at[pl.ds(p * part, part)], isem.at[p])
        for p in range(PARTS)
    ]
    hcopy = pltpu.make_async_copy(hh_ref.at[pl.ds(pl.multiple_of((me // 8) * 8, 8), 8)], hs, hsem)
    hcopy.start()
    for c in copies:
        c.start()

    barrier = pltpu.get_barrier_semaphore()
    for j in range(1, ni):
        pl.semaphore_signal(barrier, inc=1, device_id={"items": lax.rem(me + j, ni)}, device_id_type=MESH)
    for j in range(1, nu):
        pl.semaphore_signal(barrier, inc=1, device_id={"users": lax.rem(mx + j, nu)}, device_id_type=MESH)
    pl.semaphore_wait(barrier, ni + nu - 2)

    for j in range(1, chips):
        pltpu.make_async_remote_copy(
            src_ref=u_ref, dst_ref=uall.at[me], send_sem=us, recv_sem=ur,
            device_id={"items": lax.rem(chip + j, chips) * 2 + core}, device_id_type=MESH,
        ).start()
    uall[me] = u_ref[...]

    row16 = lax.broadcasted_iota(jnp.int32, (16, 128), 0)
    lane16 = lax.broadcasted_iota(jnp.int32, (16, 256), 1)

    def pick(index, rows_ref):
        def step(i, carry):
            for c in range(4):
                base = i * 64 + c * 16
                picked = []
                place = jnp.zeros((16, 128), jnp.int32)
                for j in range(16):
                    row = index(base + j)
                    tile = lax.shift_right_logical(row, 4)
                    picked.append(buf[tile])
                    place = jnp.where(row16 == j, (row & 15) + 16 * j, place)
                place = jnp.concatenate([place, place], axis=1)
                onehot = (place == lane16).astype(jnp.float32).astype(jnp.bfloat16)
                rows = jnp.dot(onehot, jnp.concatenate(picked, axis=0), preferred_element_type=jnp.float32)
                rows_ref[pl.ds(pl.multiple_of(base, 16), 16), :] = rows.astype(jnp.bfloat16)
            return carry
        lax.fori_loop(0, users // 64, step, 0)

    hcopy.wait()
    for c in copies:
        c.wait()
    pick(lambda k: jnp.minimum(jnp.maximum(ts_ref[k] - start, 0), n_rows - 1), gt)

    wait_bytes(uall.at[pl.ds(0, chips - 1)], us, ur, "items")
    for j in range(chips):
        k = lax.rem(chip + j, chips) * 2 + core
        pltpu.make_async_remote_copy(
            src_ref=uall.at[k], dst_ref=uall.at[k], send_sem=ps, recv_sem=pr,
            device_id={"items": partner}, device_id_type=MESH,
        ).start()
    hrow = lax.rem(me, 8)
    pick(lambda k: jnp.minimum(jnp.maximum(hs[hrow, k] - start, 0), n_rows - 1), gh)
    wait_bytes(uall.at[pl.ds(0, chips)], ps, pr, "items")

    for k in range(d // 16):
        two = jnp.concatenate([uall[2 * k].astype(jnp.float32), uall[2 * k + 1].astype(jnp.float32)], axis=0)
        U[16 * k:16 * k + 16, :] = (two * SHARP_HALF).astype(jnp.bfloat16)

    eye = lax.broadcasted_iota(jnp.int32, (256, 256), 0) == lax.broadcasted_iota(jnp.int32, (256, 256), 1)

    def own_scores(rows_ref):
        out = []
        for q in range(tiles):
            s = jnp.dot(rows_ref[q * 256:(q + 1) * 256, :], U[:, q * 256:(q + 1) * 256],
                        preferred_element_type=jnp.float32)
            out.append(jnp.sum(jnp.where(eye, s, 0.0), axis=0, keepdims=True))
        return jnp.concatenate(out, axis=1)

    local_t = t_ref[...] - start
    inside = (local_t >= 0) & (local_t < n_rows)
    mine = jnp.where(inside, own_scores(gt), 0.0)
    tval[...] = mine
    to_peers(tval, trecv, tsd, trc, "items", me, ni)
    trecv[me] = mine
    hscore = own_scores(gh)
    wait_bytes(trecv.at[pl.ds(0, ni - 1)], tsd, trc, "items")
    tscore = trecv[0]
    for k in range(1, ni):
        tscore = tscore + trecv[k]

    def block(i, sums):
        rows = buf[pl.ds(i * (ROWS // sub), ROWS // sub)].reshape(ROWS, d)
        out = []
        for q in range(tiles):
            s = jnp.dot(rows, U[:, q * 256:(q + 1) * 256], preferred_element_type=jnp.float32)
            y = jnp.tanh(s - tscore[:, q * 256:(q + 1) * 256]) + 1.0
            out.append(sums[q] + jnp.sum(y.reshape(ROWS // 8, 8, 256), axis=0))
        return tuple(out)

    zero = jnp.zeros((8, 256), jnp.float32)
    sums = lax.fori_loop(0, n_rows // ROWS, block, (zero,) * tiles)
    total = jnp.concatenate([jnp.sum(s, axis=0, keepdims=True) for s in sums], axis=1)
    local = 0.5 * (total - (jnp.tanh(hscore - tscore) + 1.0))
    lval[...] = local
    to_peers(lval, lrecv, lsd, lrc, "items", me, ni)
    lrecv[me] = local
    seen = jnp.max(jnp.where(h_ref[...] == t_ref[...], 1.0, 0.0), axis=0, keepdims=True)
    correction = 0.5 - 0.5 * seen
    wait_bytes(lrecv.at[pl.ds(0, ni - 1)], lsd, lrc, "items")
    count = lrecv[0]
    for k in range(1, ni):
        count = count + lrecv[k]
    rank = 1.0 + (count - correction)
    out_ref[...] = jnp.log(rank)
    hit = 1.0 / (1.0 + jnp.exp(rank - 10.5))
    gain = hit * (0.6931471805599453 / jnp.log(1.0 + rank))

    def lanes(v):
        acc = v[:, 0:128]
        for g in range(1, users // 128):
            acc = acc + v[:, g * 128:(g + 1) * 128]
        return acc

    both = jnp.concatenate([lanes(hit), lanes(gain)], axis=0)
    mval[...] = both
    to_peers(mval, mrecv, msd, mrc, "users", mx, nu)
    mrecv[mx] = both
    wait_bytes(mrecv.at[pl.ds(0, nu - 1)], msd, mrc, "users")
    met = mrecv[0]
    for k in range(1, nu):
        met = met + mrecv[k]
    met_ref[...] = jnp.sum(met, axis=1, keepdims=True) * (1.0 / (users * nu))


def body(user_emb, item_emb, target, history):
    ni = lax.axis_size("items")
    nu = lax.axis_size("users")
    users = target.shape[0]
    n_rows, d = item_emb.shape
    vmem = pl.BlockSpec(memory_space=pltpu.VMEM)
    hbm = pl.BlockSpec(memory_space=pl.ANY)
    dma = pltpu.SemaphoreType.DMA
    ht = history.T
    lr, met = pl.pallas_call(
        functools.partial(kernel, ni, nu),
        out_shape=(jax.ShapeDtypeStruct((1, users), jnp.float32), jax.ShapeDtypeStruct((2, 1), jnp.float32)),
        in_specs=[vmem, vmem, vmem, pl.BlockSpec(memory_space=pltpu.SMEM), hbm, hbm],
        out_specs=(vmem, vmem),
        scratch_shapes=[
            pltpu.VMEM((n_rows // 16, 16, d), jnp.bfloat16),
            pltpu.VMEM((ni, d // ni, users), jnp.bfloat16),
            pltpu.VMEM((d, users), jnp.bfloat16),
            pltpu.VMEM((users, d), jnp.bfloat16),
            pltpu.VMEM((users, d), jnp.bfloat16),
            pltpu.SMEM((8, users), jnp.int32),
            pltpu.VMEM((1, users), jnp.float32),
            pltpu.VMEM((1, users), jnp.float32),
            pltpu.VMEM((2, 128), jnp.float32),
            pltpu.VMEM((ni, 1, users), jnp.float32),
            pltpu.VMEM((ni, 1, users), jnp.float32),
            pltpu.VMEM((nu, 2, 128), jnp.float32),
            dma((PARTS,)), dma, dma, dma, dma, dma, dma, dma, dma, dma, dma, dma,
        ],
        compiler_params=pltpu.CompilerParams(
            collective_id=0, has_side_effects=True, vmem_limit_bytes=56 * 2**20
        ),
        name="rank_metrics",
    )(user_emb.T, target.reshape(1, users), ht, target, ht, item_emb.reshape(n_rows // 16, 16, d))
    return lr.reshape(users), met.reshape(2)


def solution(mesh):
    return jax.shard_map(
        body,
        mesh=mesh,
        in_specs=(P("users", "items"), P("items", None), P("users"), P("users", None)),
        out_specs=(P("users"), P()),
        check_vma=False,
    )
```

```python
import functools

import jax
import jax.numpy as jnp
from jax import lax
from jax.experimental import pallas as pl
from jax.experimental.pallas import tpu as pltpu
from jax.sharding import PartitionSpec as P

MESH = pl.DeviceIdType.MESH
SHARP_HALF = 2.0
ROWS = 8192
PARTS = 8


HALVES = 2


def by_distance(sides):
    steps = [()]
    for n in sides:
        steps = [s + (k,) for s in steps for k in range(n)]
    far = lambda s: sum(min(k, n - k) for k, n in zip(s, sides))
    return sorted((s for s in steps if any(s)), key=far, reverse=True)


def wait_bytes(ref, send, recv, axis):
    d = pltpu.make_async_remote_copy(
        src_ref=ref, dst_ref=ref, send_sem=send, recv_sem=recv,
        device_id={axis: 0}, device_id_type=MESH,
    )
    d.wait_recv()
    d.wait_send()


def kernel(ni, nu, u_ref, t_ref, h_ref, items_ref, out_ref, met_ref,
           buf, uall, U, gt, gh, where_v, where_s, tval, lval, mval, trecv, lrecv, mrecv,
           isem, wsem, us, ur, ps, pr, tsd, trc, lsd, lrc, msd, mrc):
    n_tiles, sub, d = buf.shape
    n_rows = n_tiles * sub
    users = t_ref.shape[1]
    half = users // HALVES
    tiles = half // 256
    me = lax.axis_index("items")
    mx = lax.axis_index("users")
    core = lax.rem(me, 2)
    chip = me // 2
    chips = ni // 2
    side = 4
    z = lax.rem(chip, side)
    y = chip // side
    partner = chip * 2 + 1 - core
    start = me * n_rows

    def peer(step):
        return (lax.rem(y + step[0], side) * side + lax.rem(z + step[1], side)) * 2 + lax.rem(core + step[2], 2)

    everyone = by_distance((ni // (2 * side), side, 2))
    same_core = [s for s in everyone if s[2] == 0]

    def to_all(src, dst, send, recv, steps):
        for s in steps:
            pltpu.make_async_remote_copy(
                src_ref=src, dst_ref=dst, send_sem=send, recv_sem=recv,
                device_id={"items": peer(s)}, device_id_type=MESH,
            ).start()

    part = n_tiles // PARTS
    copies = [
        pltpu.make_async_copy(items_ref.at[pl.ds(p * part, part)], buf.at[pl.ds(p * part, part)], isem.at[p])
        for p in range(PARTS)
    ]
    for c in copies:
        c.start()
    for k, ids in enumerate((t_ref[...], h_ref[pl.ds(me, 1), :])):
        slab, row = lax.shift_right_logical(ids, 4) & (n_tiles - 1), ids & (sub - 1)
        for g in range(users // 128):
            where_v[2 * k, g:g + 1, :] = slab[:, g * 128:(g + 1) * 128]
            where_v[2 * k + 1, g:g + 1, :] = row[:, g * 128:(g + 1) * 128]
    wcopy = pltpu.make_async_copy(where_v, where_s, wsem)

    barrier = pltpu.get_barrier_semaphore()
    for s in everyone:
        pl.semaphore_signal(barrier, inc=1, device_id={"items": peer(s)}, device_id_type=MESH)
    for j in range(1, nu):
        pl.semaphore_signal(barrier, inc=1, device_id={"users": lax.rem(mx + j, nu)}, device_id_type=MESH)
    wcopy.start()
    seen = jnp.max(jnp.where(h_ref[...] == t_ref[...], 1.0, 0.0), axis=0, keepdims=True)
    correction = 0.5 - 0.5 * seen
    pl.semaphore_wait(barrier, ni + nu - 2)

    for h in range(HALVES):
        to_all(u_ref.at[:, pl.ds(h * half, half)], uall.at[h, me], us.at[h], ur.at[h], same_core)
    for h in range(HALVES):
        uall[h, me] = u_ref[:, h * half:(h + 1) * half]

    row16 = lax.broadcasted_iota(jnp.int32, (16, 128), 0)
    lane16 = lax.broadcasted_iota(jnp.int32, (16, 256), 1) - 16 * lax.broadcasted_iota(jnp.int32, (16, 256), 0)
    chunks = 8

    def pick(which, rows_ref):
        def step(i, carry):
            for c in range(chunks):
                base = i * (16 * chunks) + c * 16
                picked = []
                place = jnp.zeros((16, 128), jnp.int32)
                for j in range(16):
                    picked.append(buf[where_s[2 * which, i, c * 16 + j]])
                    place = jnp.where(row16 == j, where_s[2 * which + 1, i, c * 16 + j], place)
                place = jnp.concatenate([place, place], axis=1)
                onehot = (place == lane16).astype(jnp.float32).astype(jnp.bfloat16)
                rows = jnp.dot(onehot, jnp.concatenate(picked, axis=0), preferred_element_type=jnp.float32)
                rows_ref[pl.ds(pl.multiple_of(base, 16), 16), :] = rows.astype(jnp.bfloat16)
            return carry
        lax.fori_loop(0, users // (16 * chunks), step, 0)

    def forward(h):
        wait_bytes(uall.at[h, pl.ds(0, chips - 1)], us.at[h], ur.at[h], "items")
        for s in same_core + [(0, 0, 0)]:
            k = peer(s)
            pltpu.make_async_remote_copy(
                src_ref=uall.at[h, k], dst_ref=uall.at[h, k], send_sem=ps.at[h], recv_sem=pr.at[h],
                device_id={"items": partner}, device_id_type=MESH,
            ).start()

    def join(h):
        wait_bytes(uall.at[h, pl.ds(0, chips)], ps.at[h], pr.at[h], "items")
        for k in range(d // 16):
            two = jnp.concatenate([uall[h, 2 * k].astype(jnp.float32), uall[h, 2 * k + 1].astype(jnp.float32)], axis=0)
            U[16 * k:16 * k + 16, h * half:(h + 1) * half] = (two * SHARP_HALF).astype(jnp.bfloat16)

    eye = lax.broadcasted_iota(jnp.int32, (256, 256), 0) == lax.broadcasted_iota(jnp.int32, (256, 256), 1)

    def own_scores(rows_ref, h):
        out = []
        for q in range(tiles * h, tiles * (h + 1)):
            s = jnp.dot(rows_ref[q * 256:(q + 1) * 256, :], U[:, q * 256:(q + 1) * 256],
                        preferred_element_type=jnp.float32)
            out.append(jnp.sum(jnp.where(eye, s, 0.0), axis=0, keepdims=True))
        return jnp.concatenate(out, axis=1)

    local_t = t_ref[...] - start
    inside = (local_t >= 0) & (local_t < n_rows)

    def send_tscore(h):
        mine = jnp.where(inside[:, h * half:(h + 1) * half], own_scores(gt, h), 0.0)
        tval[h] = mine
        to_all(tval.at[h], trecv.at[h, me], tsd.at[h], trc.at[h], everyone)
        trecv[h, me] = mine

    def total_of(recv, h, send_sem, recv_sem):
        wait_bytes(recv.at[h, pl.ds(0, ni - 1)], send_sem.at[h], recv_sem.at[h], "items")
        v = recv[h, 0]
        for k in range(1, ni):
            v = v + recv[h, k]
        return v

    def score(h, tscore, lo, hi, sums):
        def block(i, sums):
            rows = buf[pl.ds(i * (ROWS // sub), ROWS // sub)].reshape(ROWS, d)
            out = []
            for q in range(tiles):
                s = jnp.dot(rows, U[:, h * half + q * 256:h * half + (q + 1) * 256], preferred_element_type=jnp.float32)
                y = jnp.tanh(s - tscore[:, q * 256:(q + 1) * 256]) + 1.0
                out.append(sums[q] + jnp.sum(y.reshape(ROWS // 8, 8, 256), axis=0))
            return tuple(out)
        return lax.fori_loop(lo, hi, block, sums)

    def send_count(h, sums, hscore, tscore):
        total = jnp.concatenate([jnp.sum(s, axis=0, keepdims=True) for s in sums], axis=1)
        local = 0.5 * (total - (jnp.tanh(hscore - tscore) + 1.0))
        lval[h] = local
        to_all(lval.at[h], lrecv.at[h, me], lsd.at[h], lrc.at[h], everyone)
        lrecv[h, me] = local

    def lanes(v):
        acc = v[:, 0:128]
        for g in range(1, half // 128):
            acc = acc + v[:, g * 128:(g + 1) * 128]
        return acc

    def finish(h):
        count = total_of(lrecv, h, lsd, lrc)
        rank = 1.0 + (count - correction[:, h * half:(h + 1) * half])
        out_ref[:, h * half:(h + 1) * half] = jnp.log(rank)
        hit = 1.0 / (1.0 + jnp.exp(rank - 10.5))
        gain = hit * (0.6931471805599453 / jnp.log(1.0 + rank))
        return jnp.concatenate([lanes(hit), lanes(gain)], axis=0)

    zero = (jnp.zeros((8, 256), jnp.float32),) * tiles
    steps = n_rows // ROWS

    wcopy.wait()
    for c in copies:
        c.wait()
    pick(0, gt)
    forward(0)
    join(0)
    send_tscore(0)
    forward(1)
    pick(1, gh)
    hscore0 = own_scores(gh, 0)
    tscore0 = total_of(trecv, 0, tsd, trc)
    sums = score(0, tscore0, 0, steps // 2, zero)
    join(1)
    send_tscore(1)
    hscore1 = own_scores(gh, 1)
    sums = score(0, tscore0, steps // 2, steps, sums)
    send_count(0, sums, hscore0, tscore0)
    tscore1 = total_of(trecv, 1, tsd, trc)
    sums = score(1, tscore1, 0, steps, zero)
    send_count(1, sums, hscore1, tscore1)
    both = finish(0)
    both = both + finish(1)
    mval[...] = both
    for j in range(1, nu):
        pltpu.make_async_remote_copy(
            src_ref=mval, dst_ref=mrecv.at[mx], send_sem=msd, recv_sem=mrc,
            device_id={"users": lax.rem(mx + j, nu)}, device_id_type=MESH,
        ).start()
    mrecv[mx] = both
    wait_bytes(mrecv.at[pl.ds(0, nu - 1)], msd, mrc, "users")
    met = mrecv[0]
    for k in range(1, nu):
        met = met + mrecv[k]
    met_ref[...] = jnp.sum(met, axis=1, keepdims=True) * (1.0 / (users * nu))


def body(user_emb, item_emb, target, history):
    ni = lax.axis_size("items")
    nu = lax.axis_size("users")
    users = target.shape[0]
    n_rows, d = item_emb.shape
    half = users // HALVES
    vmem = pl.BlockSpec(memory_space=pltpu.VMEM)
    hbm = pl.BlockSpec(memory_space=pl.ANY)
    dma = pltpu.SemaphoreType.DMA
    ht = history.T
    lr, met = pl.pallas_call(
        functools.partial(kernel, ni, nu),
        out_shape=(jax.ShapeDtypeStruct((1, users), jnp.float32), jax.ShapeDtypeStruct((2, 1), jnp.float32)),
        in_specs=[vmem, vmem, vmem, hbm],
        out_specs=(vmem, vmem),
        scratch_shapes=[
            pltpu.VMEM((n_rows // 16, 16, d), jnp.bfloat16),
            pltpu.VMEM((HALVES, ni, d // ni, half), jnp.bfloat16),
            pltpu.VMEM((d, users), jnp.bfloat16),
            pltpu.VMEM((users, d), jnp.bfloat16),
            pltpu.VMEM((users, d), jnp.bfloat16),
            pltpu.VMEM((4, users // 128, 128), jnp.int32),
            pltpu.SMEM((4, users // 128, 128), jnp.int32),
            pltpu.VMEM((HALVES, 1, half), jnp.float32),
            pltpu.VMEM((HALVES, 1, half), jnp.float32),
            pltpu.VMEM((2, 128), jnp.float32),
            pltpu.VMEM((HALVES, ni, 1, half), jnp.float32),
            pltpu.VMEM((HALVES, ni, 1, half), jnp.float32),
            pltpu.VMEM((nu, 2, 128), jnp.float32),
            dma((PARTS,)), dma,
            dma((HALVES,)), dma((HALVES,)), dma((HALVES,)), dma((HALVES,)),
            dma((HALVES,)), dma((HALVES,)), dma((HALVES,)), dma((HALVES,)),
            dma, dma,
        ],
        compiler_params=pltpu.CompilerParams(
            collective_id=0, has_side_effects=True, vmem_limit_bytes=56 * 2**20
        ),
        name="rank_metrics",
    )(user_emb.T, target.reshape(1, users), ht, item_emb.reshape(n_rows // 16, 16, d))
    return lr.reshape(users), met.reshape(2)


def solution(mesh):
    return jax.shard_map(
        body,
        mesh=mesh,
        in_specs=(P("users", "items"), P("items", None), P("users"), P("users", None)),
        out_specs=(P("users"), P()),
        check_vma=False,
    )
```

```python
import functools

import jax
import jax.numpy as jnp
from jax import lax
from jax.experimental import pallas as pl
from jax.experimental.pallas import tpu as pltpu
from jax.sharding import PartitionSpec as P

MESH = pl.DeviceIdType.MESH
SHARP_HALF = 2.0
ROWS = 8192
PARTS = 8


HALVES = 2


def by_distance(sides):
    steps = [()]
    for n in sides:
        steps = [s + (k,) for s in steps for k in range(n)]
    far = lambda s: sum(min(k, n - k) for k, n in zip(s, sides))
    return sorted((s for s in steps if any(s)), key=far, reverse=True)


def wait_bytes(ref, send, recv, axis):
    d = pltpu.make_async_remote_copy(
        src_ref=ref, dst_ref=ref, send_sem=send, recv_sem=recv,
        device_id={axis: 0}, device_id_type=MESH,
    )
    d.wait_recv()
    d.wait_send()


def kernel(ni, nu, u_hbm, t_hbm, h_hbm, items_ref, out_ref, met_ref,
           u_ref, t_ref, h_ref,
           buf, uall, U, gt, gh, where_v, where_s, tval, lval, mval, trecv, lrecv, mrecv,
           isem, wsem, asem, us, ur, ps, pr, tsd, trc, lsd, lrc, msd, mrc):
    n_tiles, sub, d = buf.shape
    n_rows = n_tiles * sub
    users = t_ref.shape[1]
    half = users // HALVES
    tiles = half // 256
    me = lax.axis_index("items")
    mx = lax.axis_index("users")
    core = lax.rem(me, 2)
    chip = me // 2
    chips = ni // 2
    side = 4
    z = lax.rem(chip, side)
    y = chip // side
    partner = chip * 2 + 1 - core
    start = me * n_rows

    def peer(step):
        return (lax.rem(y + step[0], side) * side + lax.rem(z + step[1], side)) * 2 + lax.rem(core + step[2], 2)

    everyone = by_distance((ni // (2 * side), side, 2))
    same_core = [s for s in everyone if s[2] == 0]

    def to_all(src, dst, send, recv, steps):
        for s in steps:
            pltpu.make_async_remote_copy(
                src_ref=src, dst_ref=dst, send_sem=send, recv_sem=recv,
                device_id={"items": peer(s)}, device_id_type=MESH,
            ).start()

    small = [
        pltpu.make_async_copy(src, dst, asem.at[k])
        for k, (src, dst) in enumerate(((u_hbm, u_ref), (t_hbm, t_ref), (h_hbm, h_ref)))
    ]
    for c in small:
        c.start()
    barrier = pltpu.get_barrier_semaphore()
    for s in everyone:
        pl.semaphore_signal(barrier, inc=1, device_id={"items": peer(s)}, device_id_type=MESH)
    for j in range(1, nu):
        pl.semaphore_signal(barrier, inc=1, device_id={"users": lax.rem(mx + j, nu)}, device_id_type=MESH)
    part = n_tiles // PARTS
    copies = [
        pltpu.make_async_copy(items_ref.at[pl.ds(p * part, part)], buf.at[pl.ds(p * part, part)], isem.at[p])
        for p in range(PARTS)
    ]
    for c in copies:
        c.start()
    small[0].wait()
    pl.semaphore_wait(barrier, ni + nu - 2)

    for h in range(HALVES):
        to_all(u_ref.at[:, pl.ds(h * half, half)], uall.at[h, me], us.at[h], ur.at[h], same_core)
    for c in small[1:]:
        c.wait()
    for k, ids in enumerate((t_ref[...], h_ref[pl.ds(me, 1), :])):
        slab, row = lax.shift_right_logical(ids, 4) & (n_tiles - 1), ids & (sub - 1)
        for g in range(users // 128):
            where_v[2 * k, g:g + 1, :] = slab[:, g * 128:(g + 1) * 128]
            where_v[2 * k + 1, g:g + 1, :] = row[:, g * 128:(g + 1) * 128]
    seen = jnp.max(jnp.where(h_ref[...] == t_ref[...], 1.0, 0.0), axis=0, keepdims=True)
    correction = 0.5 - 0.5 * seen
    for h in range(HALVES):
        uall[h, me] = u_ref[:, h * half:(h + 1) * half]
    wcopy = pltpu.make_async_copy(where_v, where_s, wsem)
    wcopy.start()

    row16 = lax.broadcasted_iota(jnp.int32, (16, 128), 0)
    lane16 = lax.broadcasted_iota(jnp.int32, (16, 256), 1) - 16 * lax.broadcasted_iota(jnp.int32, (16, 256), 0)
    chunks = 8

    def pick(which, rows_ref):
        def step(i, carry):
            for c in range(chunks):
                base = i * (16 * chunks) + c * 16
                picked = []
                place = jnp.zeros((16, 128), jnp.int32)
                for j in range(16):
                    picked.append(buf[where_s[2 * which, i, c * 16 + j]])
                    place = jnp.where(row16 == j, where_s[2 * which + 1, i, c * 16 + j], place)
                place = jnp.concatenate([place, place], axis=1)
                onehot = (place == lane16).astype(jnp.float32).astype(jnp.bfloat16)
                rows = jnp.dot(onehot, jnp.concatenate(picked, axis=0), preferred_element_type=jnp.float32)
                rows_ref[pl.ds(pl.multiple_of(base, 16), 16), :] = rows.astype(jnp.bfloat16)
            return carry
        lax.fori_loop(0, users // (16 * chunks), step, 0)

    def forward(h):
        wait_bytes(uall.at[h, pl.ds(0, chips - 1)], us.at[h], ur.at[h], "items")
        for s in same_core + [(0, 0, 0)]:
            k = peer(s)
            pltpu.make_async_remote_copy(
                src_ref=uall.at[h, k], dst_ref=uall.at[h, k], send_sem=ps.at[h], recv_sem=pr.at[h],
                device_id={"items": partner}, device_id_type=MESH,
            ).start()

    def join(h):
        wait_bytes(uall.at[h, pl.ds(0, chips)], ps.at[h], pr.at[h], "items")
        for k in range(d // 16):
            two = jnp.concatenate([uall[h, 2 * k].astype(jnp.float32), uall[h, 2 * k + 1].astype(jnp.float32)], axis=0)
            U[16 * k:16 * k + 16, h * half:(h + 1) * half] = (two * SHARP_HALF).astype(jnp.bfloat16)

    eye = lax.broadcasted_iota(jnp.int32, (256, 256), 0) == lax.broadcasted_iota(jnp.int32, (256, 256), 1)

    def own_scores(rows_ref, h):
        out = []
        for q in range(tiles * h, tiles * (h + 1)):
            s = jnp.dot(rows_ref[q * 256:(q + 1) * 256, :], U[:, q * 256:(q + 1) * 256],
                        preferred_element_type=jnp.float32)
            out.append(jnp.sum(jnp.where(eye, s, 0.0), axis=0, keepdims=True))
        return jnp.concatenate(out, axis=1)

    local_t = t_ref[...] - start
    inside = (local_t >= 0) & (local_t < n_rows)

    def send_tscore(h):
        mine = jnp.where(inside[:, h * half:(h + 1) * half], own_scores(gt, h), 0.0)
        tval[h] = mine
        to_all(tval.at[h], trecv.at[h, me], tsd.at[h], trc.at[h], everyone)
        trecv[h, me] = mine

    def total_of(recv, h, send_sem, recv_sem):
        wait_bytes(recv.at[h, pl.ds(0, ni - 1)], send_sem.at[h], recv_sem.at[h], "items")
        v = recv[h, 0]
        for k in range(1, ni):
            v = v + recv[h, k]
        return v

    def score(h, tscore, lo, hi, sums):
        def block(i, sums):
            rows = buf[pl.ds(i * (ROWS // sub), ROWS // sub)].reshape(ROWS, d)
            out = []
            for q in range(tiles):
                s = jnp.dot(rows, U[:, h * half + q * 256:h * half + (q + 1) * 256], preferred_element_type=jnp.float32)
                y = jnp.tanh(s - tscore[:, q * 256:(q + 1) * 256]) + 1.0
                out.append(sums[q] + jnp.sum(y.reshape(ROWS // 8, 8, 256), axis=0))
            return tuple(out)
        return lax.fori_loop(lo, hi, block, sums)

    def send_count(h, sums, hscore, tscore):
        total = jnp.concatenate([jnp.sum(s, axis=0, keepdims=True) for s in sums], axis=1)
        local = 0.5 * (total - (jnp.tanh(hscore - tscore) + 1.0))
        lval[h] = local
        to_all(lval.at[h], lrecv.at[h, me], lsd.at[h], lrc.at[h], everyone)
        lrecv[h, me] = local

    def lanes(v):
        acc = v[:, 0:128]
        for g in range(1, half // 128):
            acc = acc + v[:, g * 128:(g + 1) * 128]
        return acc

    def finish(h):
        count = total_of(lrecv, h, lsd, lrc)
        rank = 1.0 + (count - correction[:, h * half:(h + 1) * half])
        out_ref[:, h * half:(h + 1) * half] = jnp.log(rank)
        hit = 1.0 / (1.0 + jnp.exp(rank - 10.5))
        gain = hit * (0.6931471805599453 / jnp.log(1.0 + rank))
        return jnp.concatenate([lanes(hit), lanes(gain)], axis=0)

    zero = (jnp.zeros((8, 256), jnp.float32),) * tiles
    steps = n_rows // ROWS

    wcopy.wait()
    for c in copies:
        c.wait()
    pick(0, gt)
    forward(0)
    join(0)
    send_tscore(0)
    forward(1)
    pick(1, gh)
    hscore0 = own_scores(gh, 0)
    tscore0 = total_of(trecv, 0, tsd, trc)
    sums = score(0, tscore0, 0, steps // 2, zero)
    join(1)
    send_tscore(1)
    hscore1 = own_scores(gh, 1)
    sums = score(0, tscore0, steps // 2, steps, sums)
    send_count(0, sums, hscore0, tscore0)
    tscore1 = total_of(trecv, 1, tsd, trc)
    sums = score(1, tscore1, 0, steps, zero)
    send_count(1, sums, hscore1, tscore1)
    both = finish(0)
    both = both + finish(1)
    mval[...] = both
    for j in range(1, nu):
        pltpu.make_async_remote_copy(
            src_ref=mval, dst_ref=mrecv.at[mx], send_sem=msd, recv_sem=mrc,
            device_id={"users": lax.rem(mx + j, nu)}, device_id_type=MESH,
        ).start()
    mrecv[mx] = both
    wait_bytes(mrecv.at[pl.ds(0, nu - 1)], msd, mrc, "users")
    met = mrecv[0]
    for k in range(1, nu):
        met = met + mrecv[k]
    met_ref[...] = met


def hand_over(lr_ref, met_ref, lr_out, met_out, *, scale):
    lr_out[...] = lr_ref[...]
    v = jnp.sum(met_ref[...], axis=1, keepdims=True) * scale
    met_out[...] = jnp.concatenate([v[0:1], v[1:2]], axis=1)


def body(user_emb, item_emb, target, history):
    ni = lax.axis_size("items")
    nu = lax.axis_size("users")
    users = target.shape[0]
    n_rows, d = item_emb.shape
    half = users // HALVES
    vmem = pl.BlockSpec(memory_space=pltpu.VMEM)
    hbm = pl.BlockSpec(memory_space=pl.ANY)
    dma = pltpu.SemaphoreType.DMA
    ht = history.T
    lr, met = pl.pallas_call(
        functools.partial(kernel, ni, nu),
        out_shape=(pltpu.VMEM((1, users), jnp.float32), pltpu.VMEM((2, 128), jnp.float32)),
        in_specs=[hbm, hbm, hbm, hbm],
        out_specs=(vmem, vmem),
        scratch_shapes=[
            pltpu.VMEM((d // ni, users), jnp.bfloat16),
            pltpu.VMEM((1, users), jnp.int32),
            pltpu.VMEM((ni, users), jnp.int32),
            pltpu.VMEM((n_rows // 16, 16, d), jnp.bfloat16),
            pltpu.VMEM((HALVES, ni, d // ni, half), jnp.bfloat16),
            pltpu.VMEM((d, users), jnp.bfloat16),
            pltpu.VMEM((users, d), jnp.bfloat16),
            pltpu.VMEM((users, d), jnp.bfloat16),
            pltpu.VMEM((4, users // 128, 128), jnp.int32),
            pltpu.SMEM((4, users // 128, 128), jnp.int32),
            pltpu.VMEM((HALVES, 1, half), jnp.float32),
            pltpu.VMEM((HALVES, 1, half), jnp.float32),
            pltpu.VMEM((2, 128), jnp.float32),
            pltpu.VMEM((HALVES, ni, 1, half), jnp.float32),
            pltpu.VMEM((HALVES, ni, 1, half), jnp.float32),
            pltpu.VMEM((nu, 2, 128), jnp.float32),
            dma((PARTS,)), dma, dma((3,)),
            dma((HALVES,)), dma((HALVES,)), dma((HALVES,)), dma((HALVES,)),
            dma((HALVES,)), dma((HALVES,)), dma((HALVES,)), dma((HALVES,)),
            dma, dma,
        ],
        compiler_params=pltpu.CompilerParams(
            collective_id=0, has_side_effects=True, vmem_limit_bytes=56 * 2**20
        ),
        name="rank_metrics",
    )(user_emb.T, target.reshape(1, users), ht, item_emb.reshape(n_rows // 16, 16, d))
    lr, met = pl.pallas_call(
        functools.partial(hand_over, scale=1.0 / (users * nu)),
        out_shape=(jax.ShapeDtypeStruct((1, users), jnp.float32), jax.ShapeDtypeStruct((1, 2), jnp.float32)),
        in_specs=[vmem, vmem],
        out_specs=(vmem, vmem),
        name="hand_over",
    )(*(pltpu.with_memory_space_constraint(v, pltpu.VMEM) for v in (lr, met)))
    return lr.reshape(users), met.reshape(2)


def solution(mesh):
    return jax.shard_map(
        body,
        mesh=mesh,
        in_specs=(P("users", "items"), P("items", None), P("users"), P("users", None)),
        out_specs=(P("users"), P()),
        check_vma=False,
    )
```

```python
import functools

import jax
import jax.numpy as jnp
from jax import lax
from jax.experimental import pallas as pl
from jax.experimental.pallas import tpu as pltpu
from jax.sharding import PartitionSpec as P

MESH = pl.DeviceIdType.MESH
SHARP_HALF = 2.0
ROWS = 16384
PARTS = 8


HALVES = 2


def by_distance(sides):
    steps = [()]
    for n in sides:
        steps = [s + (k,) for s in steps for k in range(n)]
    far = lambda s: sum(min(k, n - k) for k, n in zip(s, sides))
    return sorted((s for s in steps if any(s)), key=far, reverse=True)


def wait_bytes(ref, send, recv, axis):
    d = pltpu.make_async_remote_copy(
        src_ref=ref, dst_ref=ref, send_sem=send, recv_sem=recv,
        device_id={axis: 0}, device_id_type=MESH,
    )
    d.wait_recv()
    d.wait_send()


def kernel(ni, nu, u_hbm, t_hbm, h_hbm, items_ref, out_ref, met_ref,
           u_ref, t_ref, h_ref,
           buf, uall, U, gt, gh, where_v, where_s, tval, lval, mval, trecv, lrecv, mrecv,
           isem, wsem, asem, us, ur, ps, pr, tsd, trc, lsd, lrc, msd, mrc):
    n_tiles, sub, d = buf.shape
    n_rows = n_tiles * sub
    users = t_ref.shape[1]
    half = users // HALVES
    tiles = half // 256
    me = lax.axis_index("items")
    mx = lax.axis_index("users")
    core = lax.rem(me, 2)
    chip = me // 2
    chips = ni // 2
    side = 4
    z = lax.rem(chip, side)
    y = chip // side
    partner = chip * 2 + 1 - core
    start = me * n_rows

    def peer(step):
        return (lax.rem(y + step[0], side) * side + lax.rem(z + step[1], side)) * 2 + lax.rem(core + step[2], 2)

    everyone = by_distance((ni // (2 * side), side, 2))
    same_core = [s for s in everyone if s[2] == 0]

    def to_all(src, dst, send, recv, steps):
        for s in steps:
            pltpu.make_async_remote_copy(
                src_ref=src, dst_ref=dst, send_sem=send, recv_sem=recv,
                device_id={"items": peer(s)}, device_id_type=MESH,
            ).start()

    small = [
        pltpu.make_async_copy(src, dst, asem.at[k])
        for k, (src, dst) in enumerate(((u_hbm, u_ref), (t_hbm, t_ref), (h_hbm, h_ref)))
    ]
    for c in small:
        c.start()
    barrier = pltpu.get_barrier_semaphore()
    for s in everyone:
        pl.semaphore_signal(barrier, inc=1, device_id={"items": peer(s)}, device_id_type=MESH)
    for j in range(1, nu):
        pl.semaphore_signal(barrier, inc=1, device_id={"users": lax.rem(mx + j, nu)}, device_id_type=MESH)
    part = n_tiles // PARTS
    copies = [
        pltpu.make_async_copy(items_ref.at[pl.ds(p * part, part)], buf.at[pl.ds(p * part, part)], isem.at[p])
        for p in range(PARTS)
    ]
    for c in copies:
        c.start()
    small[0].wait()
    pl.semaphore_wait(barrier, ni + nu - 2)

    for h in range(HALVES):
        to_all(u_ref.at[:, pl.ds(h * half, half)], uall.at[h, me], us.at[h], ur.at[h], same_core)
    for c in small[1:]:
        c.wait()
    for k, ids in enumerate((t_ref[...], h_ref[pl.ds(me, 1), :])):
        slab, row = lax.shift_right_logical(ids, 4) & (n_tiles - 1), ids & (sub - 1)
        for g in range(users // 128):
            where_v[2 * k, g:g + 1, :] = slab[:, g * 128:(g + 1) * 128]
            where_v[2 * k + 1, g:g + 1, :] = row[:, g * 128:(g + 1) * 128]
    seen = jnp.max(jnp.where(h_ref[...] == t_ref[...], 1.0, 0.0), axis=0, keepdims=True)
    correction = 0.5 - 0.5 * seen
    for h in range(HALVES):
        uall[h, me] = u_ref[:, h * half:(h + 1) * half]
    wcopy = pltpu.make_async_copy(where_v, where_s, wsem)
    wcopy.start()

    row16 = lax.broadcasted_iota(jnp.int32, (16, 128), 0)
    lane16 = lax.broadcasted_iota(jnp.int32, (16, 256), 1) - 16 * lax.broadcasted_iota(jnp.int32, (16, 256), 0)
    chunks = 8

    def pick(which, rows_ref):
        def step(i, carry):
            for c in range(chunks):
                base = i * (16 * chunks) + c * 16
                picked = []
                place = jnp.zeros((16, 128), jnp.int32)
                for j in range(16):
                    picked.append(buf[where_s[2 * which, i, c * 16 + j]])
                    place = jnp.where(row16 == j, where_s[2 * which + 1, i, c * 16 + j], place)
                place = jnp.concatenate([place, place], axis=1)
                onehot = (place == lane16).astype(jnp.float32).astype(jnp.bfloat16)
                rows = jnp.dot(onehot, jnp.concatenate(picked, axis=0), preferred_element_type=jnp.float32)
                rows_ref[pl.ds(pl.multiple_of(base, 16), 16), :] = rows.astype(jnp.bfloat16)
            return carry
        lax.fori_loop(0, users // (16 * chunks), step, 0)

    def forward(h):
        wait_bytes(uall.at[h, pl.ds(0, chips - 1)], us.at[h], ur.at[h], "items")
        for s in same_core + [(0, 0, 0)]:
            k = peer(s)
            pltpu.make_async_remote_copy(
                src_ref=uall.at[h, k], dst_ref=uall.at[h, k], send_sem=ps.at[h], recv_sem=pr.at[h],
                device_id={"items": partner}, device_id_type=MESH,
            ).start()

    def join(h):
        wait_bytes(uall.at[h, pl.ds(0, chips)], ps.at[h], pr.at[h], "items")
        for k in range(d // 16):
            two = jnp.concatenate([uall[h, 2 * k].astype(jnp.float32), uall[h, 2 * k + 1].astype(jnp.float32)], axis=0)
            U[16 * k:16 * k + 16, h * half:(h + 1) * half] = (two * SHARP_HALF).astype(jnp.bfloat16)

    eye = lax.broadcasted_iota(jnp.int32, (256, 256), 0) == lax.broadcasted_iota(jnp.int32, (256, 256), 1)

    def own_scores(rows_ref, h):
        out = []
        for q in range(tiles * h, tiles * (h + 1)):
            s = jnp.dot(rows_ref[q * 256:(q + 1) * 256, :], U[:, q * 256:(q + 1) * 256],
                        preferred_element_type=jnp.float32)
            out.append(jnp.sum(jnp.where(eye, s, 0.0), axis=0, keepdims=True))
        return jnp.concatenate(out, axis=1)

    local_t = t_ref[...] - start
    inside = (local_t >= 0) & (local_t < n_rows)

    def send_tscore(h):
        mine = jnp.where(inside[:, h * half:(h + 1) * half], own_scores(gt, h), 0.0)
        tval[h] = mine
        to_all(tval.at[h], trecv.at[h, me], tsd.at[h], trc.at[h], everyone)
        trecv[h, me] = mine

    def total_of(recv, h, send_sem, recv_sem):
        wait_bytes(recv.at[h, pl.ds(0, ni - 1)], send_sem.at[h], recv_sem.at[h], "items")
        v = recv[h, 0]
        for k in range(1, ni):
            v = v + recv[h, k]
        return v

    def score(h, tscore, lo, hi, sums):
        def block(i, sums):
            rows = buf[pl.ds(i * (ROWS // sub), ROWS // sub)].reshape(ROWS, d)
            out = []
            for q in range(tiles):
                s = jnp.dot(rows, U[:, h * half + q * 256:h * half + (q + 1) * 256], preferred_element_type=jnp.float32)
                y = jnp.tanh(s - tscore[:, q * 256:(q + 1) * 256]) + 1.0
                out.append(sums[q] + jnp.sum(y.reshape(ROWS // 8, 8, 256), axis=0))
            return tuple(out)
        return lax.fori_loop(lo, hi, block, sums)

    def send_count(h, sums, hscore, tscore):
        total = jnp.concatenate([jnp.sum(s, axis=0, keepdims=True) for s in sums], axis=1)
        local = 0.5 * (total - (jnp.tanh(hscore - tscore) + 1.0))
        lval[h] = local
        to_all(lval.at[h], lrecv.at[h, me], lsd.at[h], lrc.at[h], everyone)
        lrecv[h, me] = local

    def lanes(v):
        acc = v[:, 0:128]
        for g in range(1, half // 128):
            acc = acc + v[:, g * 128:(g + 1) * 128]
        return acc

    def finish(h):
        count = total_of(lrecv, h, lsd, lrc)
        rank = 1.0 + (count - correction[:, h * half:(h + 1) * half])
        out_ref[:, h * half:(h + 1) * half] = jnp.log(rank)
        hit = 1.0 / (1.0 + jnp.exp(rank - 10.5))
        gain = hit * (0.6931471805599453 / jnp.log(1.0 + rank))
        return jnp.concatenate([lanes(hit), lanes(gain)], axis=0)

    zero = (jnp.zeros((8, 256), jnp.float32),) * tiles
    steps = n_rows // ROWS

    wcopy.wait()
    for c in copies:
        c.wait()
    pick(0, gt)
    forward(0)
    join(0)
    send_tscore(0)
    forward(1)
    pick(1, gh)
    join(1)
    send_tscore(1)
    hscore0 = own_scores(gh, 0)
    hscore1 = own_scores(gh, 1)
    tscore0 = total_of(trecv, 0, tsd, trc)
    sums = score(0, tscore0, 0, steps, zero)
    send_count(0, sums, hscore0, tscore0)
    tscore1 = total_of(trecv, 1, tsd, trc)
    sums = score(1, tscore1, 0, steps, zero)
    send_count(1, sums, hscore1, tscore1)
    both = finish(0)
    both = both + finish(1)
    mval[...] = both
    for j in range(1, nu):
        pltpu.make_async_remote_copy(
            src_ref=mval, dst_ref=mrecv.at[mx], send_sem=msd, recv_sem=mrc,
            device_id={"users": lax.rem(mx + j, nu)}, device_id_type=MESH,
        ).start()
    mrecv[mx] = both
    wait_bytes(mrecv.at[pl.ds(0, nu - 1)], msd, mrc, "users")
    met = mrecv[0]
    for k in range(1, nu):
        met = met + mrecv[k]
    met_ref[...] = met


def hand_over(lr_ref, met_ref, lr_out, met_out, *, scale):
    lr_out[...] = lr_ref[...]
    v = jnp.sum(met_ref[...], axis=1, keepdims=True) * scale
    met_out[...] = jnp.concatenate([v[0:1], v[1:2]], axis=1)


def body(user_emb, item_emb, target, history):
    ni = lax.axis_size("items")
    nu = lax.axis_size("users")
    users = target.shape[0]
    n_rows, d = item_emb.shape
    half = users // HALVES
    vmem = pl.BlockSpec(memory_space=pltpu.VMEM)
    hbm = pl.BlockSpec(memory_space=pl.ANY)
    dma = pltpu.SemaphoreType.DMA
    ht = history.T
    lr, met = pl.pallas_call(
        functools.partial(kernel, ni, nu),
        out_shape=(pltpu.VMEM((1, users), jnp.float32), pltpu.VMEM((2, 128), jnp.float32)),
        in_specs=[hbm, hbm, hbm, hbm],
        out_specs=(vmem, vmem),
        scratch_shapes=[
            pltpu.VMEM((d // ni, users), jnp.bfloat16),
            pltpu.VMEM((1, users), jnp.int32),
            pltpu.VMEM((ni, users), jnp.int32),
            pltpu.VMEM((n_rows // 16, 16, d), jnp.bfloat16),
            pltpu.VMEM((HALVES, ni, d // ni, half), jnp.bfloat16),
            pltpu.VMEM((d, users), jnp.bfloat16),
            pltpu.VMEM((users, d), jnp.bfloat16),
            pltpu.VMEM((users, d), jnp.bfloat16),
            pltpu.VMEM((4, users // 128, 128), jnp.int32),
            pltpu.SMEM((4, users // 128, 128), jnp.int32),
            pltpu.VMEM((HALVES, 1, half), jnp.float32),
            pltpu.VMEM((HALVES, 1, half), jnp.float32),
            pltpu.VMEM((2, 128), jnp.float32),
            pltpu.VMEM((HALVES, ni, 1, half), jnp.float32),
            pltpu.VMEM((HALVES, ni, 1, half), jnp.float32),
            pltpu.VMEM((nu, 2, 128), jnp.float32),
            dma((PARTS,)), dma, dma((3,)),
            dma((HALVES,)), dma((HALVES,)), dma((HALVES,)), dma((HALVES,)),
            dma((HALVES,)), dma((HALVES,)), dma((HALVES,)), dma((HALVES,)),
            dma, dma,
        ],
        compiler_params=pltpu.CompilerParams(
            collective_id=0, has_side_effects=True, vmem_limit_bytes=56 * 2**20
        ),
        name="rank_metrics",
    )(user_emb.T, target.reshape(1, users), ht, item_emb.reshape(n_rows // 16, 16, d))
    lr, met = pl.pallas_call(
        functools.partial(hand_over, scale=1.0 / (users * nu)),
        out_shape=(jax.ShapeDtypeStruct((1, users), jnp.float32), jax.ShapeDtypeStruct((1, 2), jnp.float32)),
        in_specs=[vmem, vmem],
        out_specs=(vmem, vmem),
        name="hand_over",
    )(*(pltpu.with_memory_space_constraint(v, pltpu.VMEM) for v in (lr, met)))
    return lr.reshape(users), met.reshape(2)


def solution(mesh):
    return jax.shard_map(
        body,
        mesh=mesh,
        in_specs=(P("users", "items"), P("items", None), P("users"), P("users", None)),
        out_specs=(P("users"), P()),
        check_vma=False,
    )
```

```python
import functools

import jax
import jax.numpy as jnp
from jax import lax
from jax.experimental import pallas as pl
from jax.experimental.pallas import tpu as pltpu
from jax.sharding import PartitionSpec as P

MESH = pl.DeviceIdType.MESH
SHARP_HALF = 2.0
ROWS = 16384
PARTS = 4


HALVES = 2


def by_distance(sides):
    steps = [()]
    for n in sides:
        steps = [s + (k,) for s in steps for k in range(n)]
    far = lambda s: sum(min(k, n - k) for k, n in zip(s, sides))
    return sorted((s for s in steps if any(s)), key=far, reverse=True)


def wait_bytes(ref, send, recv, axis):
    d = pltpu.make_async_remote_copy(
        src_ref=ref, dst_ref=ref, send_sem=send, recv_sem=recv,
        device_id={axis: 0}, device_id_type=MESH,
    )
    d.wait_recv()
    d.wait_send()


def kernel(ni, nu, u_hbm, t_hbm, h_hbm, items_ref, out_ref, met_ref,
           u_ref, t_ref, h_ref,
           buf, uall, U, gt, gh, where_v, where_s, tval, lval, mval, trecv, lrecv, mrecv,
           isem, wsem, asem, us, ur, ps, pr, tsd, trc, lsd, lrc, msd, mrc):
    n_tiles, sub, d = buf.shape
    n_rows = n_tiles * sub
    users = t_ref.shape[1]
    half = users // HALVES
    tiles = half // 256
    me = lax.axis_index("items")
    mx = lax.axis_index("users")
    core = lax.rem(me, 2)
    chip = me // 2
    chips = ni // 2
    side = 4
    z = lax.rem(chip, side)
    y = chip // side
    partner = chip * 2 + 1 - core
    start = me * n_rows

    def peer(step):
        return (lax.rem(y + step[0], side) * side + lax.rem(z + step[1], side)) * 2 + lax.rem(core + step[2], 2)

    everyone = by_distance((ni // (2 * side), side, 2))
    same_core = [s for s in everyone if s[2] == 0]

    def to_all(src, dst, send, recv, steps):
        for s in steps:
            pltpu.make_async_remote_copy(
                src_ref=src, dst_ref=dst, send_sem=send, recv_sem=recv,
                device_id={"items": peer(s)}, device_id_type=MESH,
            ).start()

    small = [
        pltpu.make_async_copy(src, dst, asem.at[k])
        for k, (src, dst) in enumerate(((u_hbm, u_ref), (t_hbm, t_ref), (h_hbm, h_ref)))
    ]
    for c in small:
        c.start()
    barrier = pltpu.get_barrier_semaphore()
    for s in everyone:
        pl.semaphore_signal(barrier, inc=1, device_id={"items": peer(s)}, device_id_type=MESH)
    for j in range(1, nu):
        pl.semaphore_signal(barrier, inc=1, device_id={"users": lax.rem(mx + j, nu)}, device_id_type=MESH)
    part = n_tiles // PARTS
    copies = [
        pltpu.make_async_copy(items_ref.at[pl.ds(p * part, part)], buf.at[pl.ds(p * part, part)], isem.at[p])
        for p in range(PARTS)
    ]
    for c in copies:
        c.start()
    small[0].wait()
    pl.semaphore_wait(barrier, ni + nu - 2)

    for h in range(HALVES):
        to_all(u_ref.at[:, pl.ds(h * half, half)], uall.at[h, me], us.at[h], ur.at[h], same_core)
    for c in small[1:]:
        c.wait()
    for k, ids in enumerate((t_ref[...], h_ref[pl.ds(me, 1), :])):
        slab, row = lax.shift_right_logical(ids, 4) & (n_tiles - 1), ids & (sub - 1)
        for g in range(users // 128):
            where_v[2 * k, g:g + 1, :] = slab[:, g * 128:(g + 1) * 128]
            where_v[2 * k + 1, g:g + 1, :] = row[:, g * 128:(g + 1) * 128]
    seen = jnp.max(jnp.where(h_ref[...] == t_ref[...], 1.0, 0.0), axis=0, keepdims=True)
    correction = 0.5 - 0.5 * seen
    for h in range(HALVES):
        uall[h, me] = u_ref[:, h * half:(h + 1) * half]
    wcopy = pltpu.make_async_copy(where_v, where_s, wsem)
    wcopy.start()

    row16 = lax.broadcasted_iota(jnp.int32, (16, 128), 0)
    lane16 = lax.broadcasted_iota(jnp.int32, (16, 256), 1) - 16 * lax.broadcasted_iota(jnp.int32, (16, 256), 0)
    chunks = 8

    def pick(which, rows_ref):
        def step(i, carry):
            for c in range(chunks):
                base = i * (16 * chunks) + c * 16
                picked = []
                place = jnp.zeros((16, 128), jnp.int32)
                for j in range(16):
                    picked.append(buf[where_s[2 * which, i, c * 16 + j]])
                    place = jnp.where(row16 == j, where_s[2 * which + 1, i, c * 16 + j], place)
                place = jnp.concatenate([place, place], axis=1)
                onehot = (place == lane16).astype(jnp.float32).astype(jnp.bfloat16)
                rows = jnp.dot(onehot, jnp.concatenate(picked, axis=0), preferred_element_type=jnp.float32)
                rows_ref[pl.ds(pl.multiple_of(base, 16), 16), :] = rows.astype(jnp.bfloat16)
            return carry
        lax.fori_loop(0, users // (16 * chunks), step, 0)

    def forward(h):
        wait_bytes(uall.at[h, pl.ds(0, chips - 1)], us.at[h], ur.at[h], "items")
        for s in same_core + [(0, 0, 0)]:
            k = peer(s)
            pltpu.make_async_remote_copy(
                src_ref=uall.at[h, k], dst_ref=uall.at[h, k], send_sem=ps.at[h], recv_sem=pr.at[h],
                device_id={"items": partner}, device_id_type=MESH,
            ).start()

    def join(h):
        wait_bytes(uall.at[h, pl.ds(0, chips)], ps.at[h], pr.at[h], "items")
        for k in range(d // 16):
            two = jnp.concatenate([uall[h, 2 * k].astype(jnp.float32), uall[h, 2 * k + 1].astype(jnp.float32)], axis=0)
            U[16 * k:16 * k + 16, h * half:(h + 1) * half] = (two * SHARP_HALF).astype(jnp.bfloat16)

    eye = lax.broadcasted_iota(jnp.int32, (256, 256), 0) == lax.broadcasted_iota(jnp.int32, (256, 256), 1)

    def own_scores(rows_ref, h):
        out = []
        for q in range(tiles * h, tiles * (h + 1)):
            s = jnp.dot(rows_ref[q * 256:(q + 1) * 256, :], U[:, q * 256:(q + 1) * 256],
                        preferred_element_type=jnp.float32)
            out.append(jnp.sum(jnp.where(eye, s, 0.0), axis=0, keepdims=True))
        return jnp.concatenate(out, axis=1)

    local_t = t_ref[...] - start
    inside = (local_t >= 0) & (local_t < n_rows)

    def send_tscore(h):
        mine = jnp.where(inside[:, h * half:(h + 1) * half], own_scores(gt, h), 0.0)
        tval[h] = mine
        to_all(tval.at[h], trecv.at[h, me], tsd.at[h], trc.at[h], everyone)
        trecv[h, me] = mine

    def total_of(recv, h, send_sem, recv_sem):
        wait_bytes(recv.at[h, pl.ds(0, ni - 1)], send_sem.at[h], recv_sem.at[h], "items")
        v = recv[h, 0]
        for k in range(1, ni):
            v = v + recv[h, k]
        return v

    def score(h, tscore, lo, hi, sums):
        def block(i, sums):
            rows = buf[pl.ds(i * (ROWS // sub), ROWS // sub)].reshape(ROWS, d)
            out = []
            for q in range(tiles):
                s = jnp.dot(rows, U[:, h * half + q * 256:h * half + (q + 1) * 256], preferred_element_type=jnp.float32)
                y = jnp.tanh(s - tscore[:, q * 256:(q + 1) * 256]) + 1.0
                out.append(sums[q] + jnp.sum(y.reshape(ROWS // 8, 8, 256), axis=0))
            return tuple(out)
        return lax.fori_loop(lo, hi, block, sums)

    def send_count(h, sums, hscore, tscore):
        total = jnp.concatenate([jnp.sum(s, axis=0, keepdims=True) for s in sums], axis=1)
        local = 0.5 * (total - (jnp.tanh(hscore - tscore) + 1.0))
        lval[h] = local
        to_all(lval.at[h], lrecv.at[h, me], lsd.at[h], lrc.at[h], everyone)
        lrecv[h, me] = local

    def lanes(v):
        acc = v[:, 0:128]
        for g in range(1, half // 128):
            acc = acc + v[:, g * 128:(g + 1) * 128]
        return acc

    def finish(h):
        count = total_of(lrecv, h, lsd, lrc)
        rank = 1.0 + (count - correction[:, h * half:(h + 1) * half])
        out_ref[:, h * half:(h + 1) * half] = jnp.log(rank)
        hit = 1.0 / (1.0 + jnp.exp(rank - 10.5))
        gain = hit * (0.6931471805599453 / jnp.log(1.0 + rank))
        return jnp.concatenate([lanes(hit), lanes(gain)], axis=0)

    zero = (jnp.zeros((8, 256), jnp.float32),) * tiles
    steps = n_rows // ROWS

    wcopy.wait()
    for c in copies:
        c.wait()
    pick(0, gt)
    forward(0)
    join(0)
    send_tscore(0)
    forward(1)
    pick(1, gh)
    join(1)
    send_tscore(1)
    hscore0 = own_scores(gh, 0)
    hscore1 = own_scores(gh, 1)
    tscore0 = total_of(trecv, 0, tsd, trc)
    sums = score(0, tscore0, 0, steps, zero)
    send_count(0, sums, hscore0, tscore0)
    tscore1 = total_of(trecv, 1, tsd, trc)
    sums = score(1, tscore1, 0, steps, zero)
    send_count(1, sums, hscore1, tscore1)
    both = finish(0)
    both = both + finish(1)
    mval[...] = both
    for j in range(1, nu):
        pltpu.make_async_remote_copy(
            src_ref=mval, dst_ref=mrecv.at[mx], send_sem=msd, recv_sem=mrc,
            device_id={"users": lax.rem(mx + j, nu)}, device_id_type=MESH,
        ).start()
    mrecv[mx] = both
    wait_bytes(mrecv.at[pl.ds(0, nu - 1)], msd, mrc, "users")
    met = mrecv[0]
    for k in range(1, nu):
        met = met + mrecv[k]
    met_ref[...] = met


def hand_over(lr_ref, met_ref, lr_out, met_out, *, scale):
    lr_out[...] = lr_ref[...]
    v = jnp.sum(met_ref[...], axis=1, keepdims=True) * scale
    met_out[...] = jnp.concatenate([v[0:1], v[1:2]], axis=1)


def body(user_emb, item_emb, target, history):
    ni = lax.axis_size("items")
    nu = lax.axis_size("users")
    users = target.shape[0]
    n_rows, d = item_emb.shape
    half = users // HALVES
    vmem = pl.BlockSpec(memory_space=pltpu.VMEM)
    hbm = pl.BlockSpec(memory_space=pl.ANY)
    dma = pltpu.SemaphoreType.DMA
    ht = history.T
    lr, met = pl.pallas_call(
        functools.partial(kernel, ni, nu),
        out_shape=(pltpu.VMEM((1, users), jnp.float32), pltpu.VMEM((2, 128), jnp.float32)),
        in_specs=[hbm, hbm, hbm, hbm],
        out_specs=(vmem, vmem),
        scratch_shapes=[
            pltpu.VMEM((d // ni, users), jnp.bfloat16),
            pltpu.VMEM((1, users), jnp.int32),
            pltpu.VMEM((ni, users), jnp.int32),
            pltpu.VMEM((n_rows // 16, 16, d), jnp.bfloat16),
            pltpu.VMEM((HALVES, ni, d // ni, half), jnp.bfloat16),
            pltpu.VMEM((d, users), jnp.bfloat16),
            pltpu.VMEM((users, d), jnp.bfloat16),
            pltpu.VMEM((users, d), jnp.bfloat16),
            pltpu.VMEM((4, users // 128, 128), jnp.int32),
            pltpu.SMEM((4, users // 128, 128), jnp.int32),
            pltpu.VMEM((HALVES, 1, half), jnp.float32),
            pltpu.VMEM((HALVES, 1, half), jnp.float32),
            pltpu.VMEM((2, 128), jnp.float32),
            pltpu.VMEM((HALVES, ni, 1, half), jnp.float32),
            pltpu.VMEM((HALVES, ni, 1, half), jnp.float32),
            pltpu.VMEM((nu, 2, 128), jnp.float32),
            dma((PARTS,)), dma, dma((3,)),
            dma((HALVES,)), dma((HALVES,)), dma((HALVES,)), dma((HALVES,)),
            dma((HALVES,)), dma((HALVES,)), dma((HALVES,)), dma((HALVES,)),
            dma, dma,
        ],
        compiler_params=pltpu.CompilerParams(
            collective_id=0, has_side_effects=True, vmem_limit_bytes=56 * 2**20
        ),
        name="rank_metrics",
    )(user_emb.T, target.reshape(1, users), ht, item_emb.reshape(n_rows // 16, 16, d))
    lr, met = pl.pallas_call(
        functools.partial(hand_over, scale=1.0 / (users * nu)),
        out_shape=(jax.ShapeDtypeStruct((1, users), jnp.float32), jax.ShapeDtypeStruct((1, 2), jnp.float32)),
        in_specs=[vmem, vmem],
        out_specs=(vmem, vmem),
        name="hand_over",
    )(*(pltpu.with_memory_space_constraint(v, pltpu.VMEM) for v in (lr, met)))
    return lr.reshape(users), met.reshape(2)


def solution(mesh):
    return jax.shard_map(
        body,
        mesh=mesh,
        in_specs=(P("users", "items"), P("items", None), P("users"), P("users", None)),
        out_specs=(P("users"), P()),
        check_vma=False,
    )
```
